128 devices in a mesh: psg: 16 (over x_hi, y, core), qry: 8 (over z, x_lo).
Axes of the slice: x: 4 (x_hi: 2, x_lo: 2; x = x_hi * 2 + x_lo), y: 4, z: 4, core: 2. Of those that a mesh axis runs over, the one named last changes fastest.
Arguments:
- hidden: bfloat16 [1024, 4096], P('qry'), may hold values from -6 to 6
- norm_gain: float32 [4096], replicated, may hold values from 0.5 to 1.5
- proj_weight: bfloat16 [4096, 4096], P('psg', 'qry'), may hold values from -0.09375 to 0.09375
- pq_codes: int32 [32768, 512], P('psg', 'qry'), may hold values from 0 to 255
- codebook: bfloat16 [512, 8, 256], P('qry'), may hold values from -560 to 560
- positives: int32 [1024], replicated, may hold values from 0 to 32767
Outputs:
- losses: float32 [1024], P('qry')
- hidden_grad: bfloat16 [1024, 4096], P('qry')
- weight_grad: float32 [4096, 4096], P('psg', 'qry')
- codebook_grad: float32 [512, 8, 256], P('qry')
The draws below stay inside these ranges and needn't reach their ends.
All inputs are finite; a program needn't handle non-finite values.
Results may differ from the reference program's by a relative error of at most 0.019.
The reference program's roundings to bfloat16 on the way (of `normed`, `queries`, `passages`, `score_grad`, `query_grad` and `passage_grad`) count: a program that leaves them out, or rounds other values in their place, can miss the bound.
Values may be sent and summed in bfloat16 or wider, within the bound.
A program may use at most 128 MiB of HBM per device.

```python
import math
import jax
import jax.numpy as jnp
from jax import lax

D = 4096
SUB = 8
K = 256
M = 512
Q = 1024
PSG_TOTAL = 32768
N_QRY = 8


def draw_codebook(key, part):
    first_key, second_key = jax.random.split(jax.random.fold_in(key, 11), 2)
    root = math.sqrt(D)
    centre_scale = 1280.0 / root
    noise_scale = 48.0 / root
    centre = jnp.clip(jax.random.normal(first_key, (M, SUB, 1), jnp.float32), -3.0, 3.0) * centre_scale
    noise = jnp.clip(jax.random.normal(second_key, (M, SUB, K), jnp.float32), -4.0, 4.0) * noise_scale
    return jnp.clip(centre + noise, -560.0, 560.0).astype(jnp.bfloat16)


def place_ends(entries, own_key, low, largest):
    longest = entries.shape.index(max(entries.shape))
    spots = []
    for shift in (0, 1):
        where = [jax.random.randint(jax.random.fold_in(own_key, axis), (), 0, length) for axis, length in enumerate(entries.shape)]
        where[longest] = (where[longest] + shift) % entries.shape[longest]
        spots.append(tuple(where))
    return entries.at[spots[0]].set(low).at[spots[1]].set(largest)


def steps_of(own_key, shape, cuts, low, high):
    factor_of, own = 1.0, jax.random.fold_in(own_key, 6)
    for position, shards_of in cuts:
        heights = jnp.exp(jax.random.uniform(jax.random.fold_in(own, position), (shards_of,), jnp.float32, low / len(cuts), high / len(cuts)))
        factor_of = factor_of * jnp.repeat(heights, shape[position] // shards_of).reshape([-1 if axis == position else 1 for axis in range(len(shape))])
    return factor_of


def normal_values(stream_key, dims, deviation, reach, pieces=(), kind=jnp.bfloat16):
    result = deviation * jax.random.normal(stream_key, dims, jnp.float32)
    if pieces:
        result = result * steps_of(stream_key, dims, pieces, -0.22, 0.18)
    return jnp.clip(result, -reach, reach).astype(kind)


def setup_inputs(seed: int = 0) -> dict:
    key_list = jax.random.split(jax.random.key(seed), 7)
    return {
        "hidden": normal_values(key_list[0], (Q, D), 1.0, 6.0, ((0, 8),)),
        "norm_gain": jnp.clip(1.0 + 0.1 * jax.random.normal(key_list[1], (D,), jnp.float32), 0.5, 1.5),
        "proj_weight": normal_values(key_list[2], (D, D), D ** -0.5, 0.09375, ((0, 16), (1, 8))),
        "pq_codes": place_ends(jax.random.randint(key_list[3], (PSG_TOTAL, M), 0, K), jax.random.fold_in(key_list[3], 1), 0, K - 1).astype(jnp.int32),
        "codebook": draw_codebook(jax.random.fold_in(key_list[6], 71), 0),
        "positives": place_ends(jax.random.randint(key_list[5], (Q,), 0, PSG_TOTAL), jax.random.fold_in(key_list[5], 1), 0, PSG_TOTAL - 1).astype(jnp.int32),
    }


score_scale = 0.0625
norm_eps = 1e-06

def reference(hidden, norm_gain, proj_weight, pq_codes, codebook, positives):
    floats_in = hidden.astype(jnp.float32)
    inverse = lax.rsqrt(lax.optimization_barrier(jnp.mean(floats_in * floats_in, axis=1, keepdims=True)) + norm_eps)
    normed = (floats_in * inverse * norm_gain[None, :]).astype(jnp.bfloat16)
    queries = jnp.dot(normed, proj_weight, preferred_element_type=jnp.float32).astype(jnp.bfloat16)
    code_table = jnp.transpose(codebook, (0, 2, 1))
    subspace = jnp.arange(M, dtype=jnp.int32)
    passages = code_table[subspace[None, :], pq_codes].reshape(pq_codes.shape[0], D)
    scores = lax.dot_general(queries, passages, (((1,), (1,)), ((), ())), preferred_element_type=jnp.float32) * score_scale
    row_max = lax.optimization_barrier(jnp.max(scores, axis=1, keepdims=True))
    expands = jnp.exp(scores - row_max)
    row_total = lax.optimization_barrier(jnp.sum(expands, axis=1, keepdims=True))
    target = jnp.arange(pq_codes.shape[0], dtype=jnp.int32)[None, :] == positives[:, None]
    positive_score = lax.optimization_barrier(jnp.sum(jnp.where(target, scores, 0.0), axis=1))
    losses = jnp.log(row_total[:, 0]) + row_max[:, 0] - positive_score
    score_grad = (expands / row_total - target.astype(jnp.float32)).astype(jnp.bfloat16)
    query_grad = (jnp.dot(score_grad, passages, preferred_element_type=jnp.float32) * score_scale).astype(jnp.bfloat16)
    passage_grad = (lax.dot_general(score_grad, queries, (((0,), (0,)), ((), ())), preferred_element_type=jnp.float32) * score_scale).astype(jnp.bfloat16)
    segment_ids = (subspace[None, :] * K + pq_codes).reshape(-1).astype(jnp.int32)
    flattened = passage_grad.astype(jnp.float32).reshape(-1, SUB)
    book_sum = jax.ops.segment_sum(flattened, segment_ids, num_segments=M * K)
    codebook_grad = jnp.transpose(book_sum.reshape(M, K, SUB), (0, 2, 1))
    weight_grad = lax.dot_general(normed, query_grad, (((0,), (0,)), ((), ())), preferred_element_type=jnp.float32)
    block_width = D // N_QRY
    norm_back = jnp.zeros((hidden.shape[0], D), jnp.float32)
    for column_group in range(N_QRY):
        low_edge = column_group * block_width
        product = lax.dot_general(query_grad[:, low_edge:low_edge + block_width], proj_weight[:, low_edge:low_edge + block_width], (((1,), (1,)), ((), ())), preferred_element_type=jnp.float32)
        norm_back = norm_back + lax.optimization_barrier(product.astype(jnp.bfloat16)).astype(jnp.float32)
    scaled = norm_back * norm_gain[None, :]
    hidden_grad = (inverse * scaled - floats_in * inverse * inverse * inverse * lax.optimization_barrier(jnp.mean(scaled * floats_in, axis=1, keepdims=True))).astype(jnp.bfloat16)
    return (losses, hidden_grad, weight_grad, codebook_grad)
```

```python
import jax
import jax.numpy as jnp
from jax import lax
from jax.experimental import pallas as pl
from jax.experimental.pallas import tpu as pltpu
from jax.sharding import Mesh
from jax.sharding import PartitionSpec as P

AXES = ("xh", "y", "k", "z", "xl")
PSG = ("xh", "y", "k")
QRY = ("z", "xl")

score_scale = 0.0625
norm_eps = 1e-06


def decode_kernel(codes_ref, book_ref, out_ref):
    subs, count = codes_ref.shape
    for tile in range(count // 128):
        block = codes_ref[:, tile * 128:(tile + 1) * 128].astype(jnp.float32).astype(jnp.int32)
        found = []
        for m in range(subs):
            code = jnp.broadcast_to(block[m:m + 1, :], (8, 128))
            low = code & 127
            first = jnp.take_along_axis(book_ref[m * 8:m * 8 + 8, 0:128].astype(jnp.float32), low, axis=1, mode="promise_in_bounds")
            second = jnp.take_along_axis(book_ref[m * 8:m * 8 + 8, 128:256].astype(jnp.float32), low, axis=1, mode="promise_in_bounds")
            found.append(jnp.where(code >= 128, second, first))
        for m in range(0, subs, 2):
            out_ref[m * 8:m * 8 + 16, tile * 128:(tile + 1) * 128] = jnp.concatenate(found[m:m + 2], 0).astype(jnp.bfloat16)

def decode(codes, book):
    subs, count = codes.shape
    step = 16
    return pl.pallas_call(
        decode_kernel,
        grid=(subs // step,),
        in_specs=[pl.BlockSpec((step, count), lambda i: (i, 0)), pl.BlockSpec((step * 8, 256), lambda i: (i, 0))],
        out_specs=pl.BlockSpec((step * 8, count), lambda i: (i, 0)),
        out_shape=jax.ShapeDtypeStruct((subs * 8, count), jnp.bfloat16),
        name="decode",
    )(codes, book)

def book_kernel(codes_ref, queries_ref, sg_ref, out_ref, pg_ref, hot_ref, gw_ref):
    count = codes_ref.shape[1]
    pg_ref[...] = (lax.dot_general(queries_ref[...], sg_ref[...], (((0,), (0,)), ((), ())), preferred_element_type=jnp.float32) * 0.0625).astype(jnp.bfloat16)
    levels = lax.broadcasted_iota(jnp.int32, (64, 128), 0)
    for group in range(4):
        for tile in range(count // 128):
            at = slice(tile * 128, (tile + 1) * 128)
            block = codes_ref[group * 8:group * 8 + 8, at].astype(jnp.float32).astype(jnp.int32)
            for m in range(8):
                row = block[m:m + 1, :]
                hi = jnp.broadcast_to(row & 63, (64, 128))
                hot_ref[m * 64:m * 64 + 64, at] = (hi == levels).astype(jnp.float32).astype(jnp.bfloat16)
                lo = jnp.broadcast_to(row >> 6, (8, 128))
                grad = pg_ref[group * 64 + m * 8:group * 64 + m * 8 + 8, at].astype(jnp.float32)
                parts = [jnp.where(lo == t, grad, 0.0) for t in range(4)]
                gw_ref[m * 32:m * 32 + 32, at] = jnp.concatenate(parts, 0).astype(jnp.bfloat16)
        full = lax.dot_general(hot_ref[...], gw_ref[...], (((1,), (1,)), ((), ())), preferred_element_type=jnp.float32)
        own = lax.broadcasted_iota(jnp.int32, (64, 256), 1) // 32
        total = jnp.zeros((64, 256), jnp.float32)
        for m in range(8):
            total = jnp.where(own == m, full[m * 64:m * 64 + 64, :], total)
        out_ref[group] = total

def book_sums(codes, queries, sg):
    subs, count = codes.shape
    rows = queries.shape[0]
    return pl.pallas_call(
        book_kernel,
        grid=(subs // 32,),
        in_specs=[pl.BlockSpec((32, count), lambda i: (i, 0)), pl.BlockSpec((rows, 256), lambda i: (0, i)), pl.BlockSpec((rows, count), lambda i: (0, 0))],
        out_specs=pl.BlockSpec((4, 64, 256), lambda i: (i, 0, 0)),
        out_shape=jax.ShapeDtypeStruct((subs // 8, 64, 256), jnp.float32),
        scratch_shapes=[pltpu.VMEM((256, count), jnp.bfloat16), pltpu.VMEM((512, count), jnp.bfloat16), pltpu.VMEM((256, count), jnp.bfloat16)],
        name="book_sums",
    )(codes, queries, sg)


def unfold(sums):
    groups = sums.shape[0]
    parts = sums.reshape(groups, 64, 8, 4, 8)
    return parts.transpose(0, 2, 4, 3, 1).reshape(groups * 8, 8, 256)


def per_device(hidden, norm_gain, proj_weight, pq_codes, codebook, positives):
    xh, y, k = (lax.axis_index(a) for a in PSG)
    psg = (xh * 4 + y) * 2 + k
    qry = lax.axis_index("z") * 2 + lax.axis_index("xl")
    own_rows, width = hidden.shape
    row_span, columns = proj_weight.shape
    subs = pq_codes.shape[1]
    half = subs // 2
    held = pq_codes.shape[0]
    piece = held // 8

    floats = hidden.astype(jnp.float32)
    inverse = lax.rsqrt(jnp.mean(floats * floats, axis=1, keepdims=True) + norm_eps)
    normed_own = (floats * inverse * norm_gain[None, :]).astype(jnp.bfloat16)
    slice_own = lax.dynamic_slice_in_dim(normed_own, psg * row_span, row_span, 1)
    normed = lax.all_gather(slice_own, QRY, axis=0, tiled=True)

    codes = pq_codes.T.astype(jnp.bfloat16)
    codes = lax.all_to_all(codes, QRY, split_axis=1, concat_axis=0, tiled=True)
    codes = codes.reshape(8, 2, half, piece).transpose(1, 0, 2, 3).reshape(2, 8 * half, piece)
    codes = lax.all_to_all(codes, "k", split_axis=0, concat_axis=2, tiled=True)[0]
    codes = lax.all_gather(codes, "y", axis=1, tiled=True)
    book_half = lax.dynamic_slice_in_dim(codebook, k * half, half, 0).reshape(half * 8, 256)
    book = lax.all_gather(book_half, QRY, axis=0, tiled=True)
    passages = decode(codes, book)

    part = jnp.dot(normed, proj_weight, preferred_element_type=jnp.float32)
    part = lax.psum_scatter(part, "k", scatter_dimension=1, tiled=True)
    part = lax.psum_scatter(part, "y", scatter_dimension=0, tiled=True)
    part = lax.psum_scatter(part, "xh", scatter_dimension=0, tiled=True)
    queries = lax.all_gather(part.astype(jnp.bfloat16), "xh", axis=0, tiled=True)
    queries = lax.all_gather(queries, QRY, axis=1, tiled=True)

    partial_value = jnp.dot(queries, passages, preferred_element_type=jnp.float32)
    scores = lax.psum_scatter(partial_value, "k", scatter_dimension=0, tiled=True) * score_scale

    block = y * 2 + k
    targets = lax.dynamic_slice_in_dim(positives, block * own_rows, own_rows, 0)
    shard = targets // held
    inside = targets - shard * held
    sixth = inside // piece
    here = (shard // 8 == xh) & (sixth == qry)
    column = jnp.where(here, (shard % 8) * piece + inside % piece, -1)
    target = lax.broadcasted_iota(jnp.int32, scores.shape, 1) == column[:, None]
    local_max = jnp.max(scores, axis=1)
    positive_part = jnp.sum(jnp.where(target, scores, 0.0), axis=1)
    local_total = jnp.sum(jnp.exp(scores - local_max[:, None]), axis=1)
    stats = lax.all_gather(
        jnp.stack([local_max, local_total, positive_part]), ("xh", "z", "xl"), axis=0
    )
    row_max = jnp.max(stats[:, 0], axis=0)
    row_total = jnp.sum(stats[:, 1] * jnp.exp(stats[:, 0] - row_max[None, :]), axis=0)
    positive_score = jnp.sum(stats[:, 2], axis=0)
    block_losses = jnp.log(row_total) + row_max - positive_score
    losses = lax.all_gather(block_losses, ("y", "k"), axis=0)
    losses = lax.dynamic_index_in_dim(losses, qry, 0, keepdims=False)
    score_grad = (
        jnp.exp(scores - row_max[:, None]) / row_total[:, None] - target.astype(jnp.float32)
    ).astype(jnp.bfloat16)
    all_grad = lax.all_gather(score_grad, "k", axis=0, tiled=True)

    query_part = lax.dot_general(
        all_grad, passages, (((1,), (1,)), ((), ())), preferred_element_type=jnp.float32
    )
    query_part = lax.psum_scatter(query_part, QRY, scatter_dimension=1, tiled=True)
    query_part = lax.psum_scatter(query_part, "xh", scatter_dimension=0, tiled=True)
    query_piece = (query_part * score_scale).astype(jnp.bfloat16)
    query_grad = lax.all_gather(query_piece, "k", axis=1, tiled=True)
    query_grad = lax.all_gather(query_grad, ("y", "xh"), axis=0, tiled=True)

    sums = book_sums(codes, queries, all_grad).astype(jnp.bfloat16)
    sums = lax.psum_scatter(sums, QRY, scatter_dimension=0, tiled=True)
    sums = lax.psum(sums, ("xh", "y"))
    sums = lax.all_gather(sums, "k", axis=0, tiled=True)
    codebook_grad = unfold(sums.astype(jnp.float32))

    weight_grad = lax.dot_general(
        normed, query_grad, (((0,), (0,)), ((), ())), preferred_element_type=jnp.float32
    )
    norm_part = lax.dot_general(
        query_grad, proj_weight, (((1,), (1,)), ((), ())), preferred_element_type=jnp.float32
    ).astype(jnp.bfloat16)
    blocks = lax.all_to_all(
        norm_part.reshape(8, own_rows, row_span), QRY, split_axis=0, concat_axis=0, tiled=True
    )
    norm_piece = jnp.sum(blocks.astype(jnp.float32), axis=0).astype(jnp.bfloat16)
    norm_back = lax.all_gather(norm_piece, PSG, axis=1, tiled=True).astype(jnp.float32)
    scaled = norm_back * norm_gain[None, :]
    hidden_grad = (
        inverse * scaled
        - floats
        * inverse
        * inverse
        * inverse
        * jnp.mean(scaled * floats, axis=1, keepdims=True)
    ).astype(jnp.bfloat16)
    return (losses, hidden_grad, weight_grad, codebook_grad)


def solution(mesh):
    split = Mesh(mesh.devices.reshape(2, 4, 2, 4, 2), AXES)
    return jax.shard_map(
        per_device,
        mesh=split,
        in_specs=(P(QRY, None), P(), P(PSG, QRY), P(PSG, QRY), P(QRY, None, None), P()),
        out_specs=(P(QRY), P(QRY, None), P(PSG, QRY), P(QRY, None, None)),
        check_vma=False,
    )
```

```python
import jax
import jax.numpy as jnp
from jax import lax
from jax.experimental import pallas as pl
from jax.experimental.pallas import tpu as pltpu
from jax.sharding import Mesh
from jax.sharding import PartitionSpec as P

AXES = ("xh", "y", "k", "z", "xl")
PSG = ("xh", "y", "k")
QRY = ("z", "xl")

score_scale = 0.0625
norm_eps = 1e-06


def decode_kernel(codes_ref, book_ref, out_ref):
    subs, count = codes_ref.shape
    for tile in range(count // 128):
        block = codes_ref[:, tile * 128:(tile + 1) * 128].astype(jnp.float32).astype(jnp.int32)
        found = []
        for m in range(subs):
            code = jnp.broadcast_to(block[m:m + 1, :], (8, 128))
            low = code & 127
            first = jnp.take_along_axis(book_ref[m * 8:m * 8 + 8, 0:128].astype(jnp.float32), low, axis=1, mode="promise_in_bounds")
            second = jnp.take_along_axis(book_ref[m * 8:m * 8 + 8, 128:256].astype(jnp.float32), low, axis=1, mode="promise_in_bounds")
            found.append(jnp.where(code >= 128, second, first))
        for m in range(0, subs, 2):
            out_ref[m * 8:m * 8 + 16, tile * 128:(tile + 1) * 128] = jnp.concatenate(found[m:m + 2], 0).astype(jnp.bfloat16)

def decode(codes, book):
    subs, count = codes.shape
    step = 16
    return pl.pallas_call(
        decode_kernel,
        grid=(subs // step,),
        in_specs=[pl.BlockSpec((step, count), lambda i: (i, 0)), pl.BlockSpec((step * 8, 256), lambda i: (i, 0))],
        out_specs=pl.BlockSpec((step * 8, count), lambda i: (i, 0)),
        out_shape=jax.ShapeDtypeStruct((subs * 8, count), jnp.bfloat16),
        name="decode",
    )(codes, book)

def book_kernel(codes_ref, queries_ref, sg_ref, out_ref, pg_ref, hot_ref, gw_ref):
    count = codes_ref.shape[1]
    pg_ref[...] = (lax.dot_general(queries_ref[...], sg_ref[...], (((0,), (0,)), ((), ())), preferred_element_type=jnp.float32) * 0.0625).astype(jnp.bfloat16)
    levels = lax.broadcasted_iota(jnp.int32, (64, 128), 0)
    for group in range(4):
        for tile in range(count // 128):
            at = slice(tile * 128, (tile + 1) * 128)
            block = codes_ref[group * 8:group * 8 + 8, at].astype(jnp.float32).astype(jnp.int32)
            for m in range(8):
                row = block[m:m + 1, :]
                hi = jnp.broadcast_to(row & 63, (64, 128))
                hot_ref[m * 64:m * 64 + 64, at] = (hi == levels).astype(jnp.float32).astype(jnp.bfloat16)
                lo = jnp.broadcast_to(row >> 6, (8, 128))
                grad = pg_ref[group * 64 + m * 8:group * 64 + m * 8 + 8, at].astype(jnp.float32)
                parts = [jnp.where(lo == t, grad, 0.0) for t in range(4)]
                gw_ref[m * 32:m * 32 + 32, at] = jnp.concatenate(parts, 0).astype(jnp.bfloat16)
        full = lax.dot_general(hot_ref[...], gw_ref[...], (((1,), (1,)), ((), ())), preferred_element_type=jnp.float32)
        own = lax.broadcasted_iota(jnp.int32, (64, 256), 1) // 32
        total = jnp.zeros((64, 256), jnp.float32)
        for m in range(8):
            total = jnp.where(own == m, full[m * 64:m * 64 + 64, :], total)
        out_ref[group] = total

def book_sums(codes, queries, sg):
    subs, count = codes.shape
    rows = queries.shape[0]
    return pl.pallas_call(
        book_kernel,
        grid=(subs // 32,),
        in_specs=[pl.BlockSpec((32, count), lambda i: (i, 0)), pl.BlockSpec((rows, 256), lambda i: (0, i)), pl.BlockSpec((rows, count), lambda i: (0, 0))],
        out_specs=pl.BlockSpec((4, 64, 256), lambda i: (i, 0, 0)),
        out_shape=jax.ShapeDtypeStruct((subs // 8, 64, 256), jnp.float32),
        scratch_shapes=[pltpu.VMEM((256, count), jnp.bfloat16), pltpu.VMEM((512, count), jnp.bfloat16), pltpu.VMEM((256, count), jnp.bfloat16)],
        name="book_sums",
    )(codes, queries, sg)


def ring(c, step):
    return lax.rem(c + (step + 4), 4)


class Place:
    def __init__(self):
        self.xh, self.y, self.k, self.z, self.xl = (lax.axis_index(a) for a in AXES)
        self.x = self.xh * 2 + self.xl
        self.qry = self.z * 2 + self.xl

    def along_x(self, step):
        x = ring(self.x, step)
        return {"xh": lax.div(x, 2), "xl": lax.rem(x, 2)}

    def along_y(self, step):
        return {"y": ring(self.y, step)}

    def along_z(self, step):
        return {"z": ring(self.z, step)}

    def core(self):
        return {"k": 1 - self.k}

    def far_x(self):
        return {"xh": 1 - self.xh}

    def group(self):
        return [
            {"z": ring(self.z, s), "xl": lax.rem(self.xl + f, 2)}
            for s in range(4)
            for f in range(2)
            if s or f
        ]


def greet(peers):
    barrier = pltpu.get_barrier_semaphore()
    for peer in peers:
        pl.semaphore_signal(
            barrier, inc=1, device_id=peer, device_id_type=pl.DeviceIdType.MESH
        )
    pl.semaphore_wait(barrier, len(peers))


class Wires:
    def __init__(self, send_sems, recv_sems):
        self.send_sems, self.recv_sems, self.copies = send_sems, recv_sems, []

    def send(self, src, dst, peer):
        n = len(self.copies)
        copy = pltpu.make_async_remote_copy(
            src_ref=src,
            dst_ref=dst,
            send_sem=self.send_sems.at[n],
            recv_sem=self.recv_sems.at[n],
            device_id=peer,
            device_id_type=pl.DeviceIdType.MESH,
        )
        copy.start()
        self.copies.append(copy)
        return copy

    def drain(self):
        for copy in self.copies:
            copy.wait_send()


def ring_gather(wires, along, own, block, halves):
    first = (wires.send(own, block(0), along(1)), wires.send(own, block(0), along(-1)))

    def forward():
        first[0].wait_recv()
        up = wires.send(halves(block(-1), 0), halves(block(-1), 0), along(1))
        first[1].wait_recv()
        down = wires.send(halves(block(1), 1), halves(block(1), 1), along(-1))

        def finish():
            up.wait_recv()
            down.wait_recv()

        return finish

    return forward


def torus_gather(wires, one, two, own, block, halves):
    forward = ring_gather(wires, one, own, lambda i: block(i, 0), halves)
    rest = [ring_gather(wires, two, own, lambda j: block(0, j), halves)]
    yield
    finish = forward()
    for i in (-1, 1):
        rest.append(
            ring_gather(wires, two, block(i, 0), lambda j, i=i: block(i, j), halves)
        )
    yield
    ends = [rest[0]()]
    finish()
    rest.append(ring_gather(wires, two, block(2, 0), lambda j: block(2, j), halves))
    yield
    ends += [r() for r in rest[1:3]]
    yield
    ends.append(rest[3]())
    for end in ends:
        end()


def run_together(*parts):
    live = list(parts)
    while live:
        live = [p for p in live if next(p, live) is not live]


def both(*parts):
    live = list(parts)
    while live:
        live = [p for p in live if next(p, live) is not live]
        yield


def psg_gather(wires, at, own, block):
    def halves(ref, side):
        rows = ref.shape[0] // 2
        return ref.at[rows * side : rows * side + rows]

    def near(s):
        return block(at.xh, ring(at.y, s), at.k)

    def far(s):
        return block(1 - at.xh, ring(at.y, s), at.k)

    across = wires.send(own, near(0), at.far_x())
    forward = ring_gather(wires, at.along_y, own, near, halves)
    cores = [wires.send(own, near(0), at.core())]
    yield
    across.wait_recv()
    forward_far = ring_gather(wires, at.along_y, far(0), far, halves)
    cores.append(wires.send(far(0), far(0), at.core()))
    yield
    finish = forward()
    for s in (-1, 1):
        cores.append(wires.send(near(s), near(s), at.core()))
    yield
    finish_far = forward_far()
    for s in (-1, 1):
        cores.append(wires.send(far(s), far(s), at.core()))
    yield
    finish()
    cores.append(wires.send(near(2), near(2), at.core()))
    finish_far()
    cores.append(wires.send(far(2), far(2), at.core()))
    for copy in cores:
        copy.wait_recv()


def rows_half(ref, side):
    rows = ref.shape[-2] // 2
    return ref.at[rows * side : rows * side + rows]


def exchange_kernel(
    slice_ref, weight_ref, codes_ref, book_ref,
    normed_ref, queries_ref, codes_all_ref, book_all_ref,
    other_ref, came_ref, acc_ref, up_ref, down_ref, from_up_ref, from_down_ref, far_ref, piece_ref,
    send_sems, recv_sems,
):
    at = Place()
    wires = Wires(send_sems, recv_sems)
    group = at.group()
    greet(
        group
        + [{"k": 1 - at.k, **g} for g in group]
        + [at.core(), at.along_y(1), at.along_y(-1), at.far_x()]
        + [{"xh": 1 - at.xh, "xl": 1 - at.xl}]
    )
    sent = []
    mine = pl.ds(pl.multiple_of(at.y * 512 + at.k * 256, 256), 256)
    rows_here = pl.ds(pl.multiple_of(at.qry * 32, 32), 32)
    for cross in range(2):
        k = at.k if cross == 0 else 1 - at.k
        rows_there = pl.ds(pl.multiple_of(k * 32, 32), 32)
        for peer in ([] if cross == 0 else [{}]) + group:
            q = peer["z"] * 2 + peer["xl"] if peer else at.qry
            sent.append(
                wires.send(
                    codes_ref.at[rows_there, pl.ds(pl.multiple_of(q * 256, 256), 256)],
                    codes_all_ref.at[rows_here, mine],
                    {"k": k, **peer},
                )
            )
    codes_all_ref[rows_here, mine] = codes_ref[
        pl.ds(pl.multiple_of(at.k * 32, 32), 32),
        pl.ds(pl.multiple_of(at.qry * 256, 256), 256),
    ]

    def column(ref, flip):
        return lambda s: ref.at[ring(at.z, s) * 2 + (at.xl if flip == 0 else 1 - at.xl)]

    partner = {"xl": 1 - at.xl}
    gathers = []
    for own, out in ((slice_ref, normed_ref), (book_ref, book_all_ref)):
        side = wires.send(own, out.at[at.qry], partner)
        gathers.append((side, out, ring_gather(wires, at.along_z, own, column(out, 0), rows_half)))
    normed_ref[at.qry] = slice_ref[...]
    book_all_ref[at.qry] = book_ref[...]
    ends = []
    for side, out, forward in gathers:
        side.wait_recv()
        far = column(out, 1)
        second = ring_gather(wires, at.along_z, far(0), far, rows_half)
        ends.append((forward(), second))
    normed_end = ends[0][1]()
    ends[0][0]()
    normed_end()

    order = (2, 1, -1, 0)
    crossed = []
    for s in order:
        b = ring(at.y, s)
        left = normed_ref[pl.ds(b * 2, 2)].reshape(256, 256)
        other_ref[b] = jnp.dot(
            left,
            weight_ref[:, pl.ds(pl.multiple_of((1 - at.k) * 256, 256), 256)],
            preferred_element_type=jnp.float32,
        )
        crossed.append(wires.send(other_ref.at[b], came_ref.at[b], at.core()))
    for s in order:
        b = ring(at.y, s)
        left = normed_ref[pl.ds(b * 2, 2)].reshape(256, 256)
        acc_ref[b] = jnp.dot(
            left,
            weight_ref[:, pl.ds(pl.multiple_of(at.k * 256, 256), 256)],
            preferred_element_type=jnp.float32,
        )
    far_y, next_y, last_y = ring(at.y, 2), ring(at.y, 1), ring(at.y, -1)
    crossed[0].wait_recv()
    acc_ref[far_y] = acc_ref[far_y] + came_ref[far_y]
    up = wires.send(acc_ref.at[far_y, 0:128], up_ref, at.along_y(1))
    down = wires.send(acc_ref.at[far_y, 128:256], down_ref, at.along_y(-1))
    crossed[1].wait_recv()
    acc_ref[next_y] = acc_ref[next_y] + came_ref[next_y]
    crossed[2].wait_recv()
    acc_ref[last_y] = acc_ref[last_y] + came_ref[last_y]
    crossed[3].wait_recv()
    acc_ref[at.y] = acc_ref[at.y] + came_ref[at.y]
    up.wait_recv()
    acc_ref[next_y, 0:128] = acc_ref[next_y, 0:128] + up_ref[...]
    up = wires.send(acc_ref.at[next_y], from_up_ref, at.along_y(1))
    down.wait_recv()
    acc_ref[last_y, 128:256] = acc_ref[last_y, 128:256] + down_ref[...]
    down = wires.send(acc_ref.at[last_y], from_down_ref, at.along_y(-1))

    for copy in sent:
        copy.wait_recv()

    def chunk(s):
        return codes_all_ref.at[:, pl.ds(pl.multiple_of(ring(at.y, s) * 512, 512), 512)]

    codes_forward = ring_gather(wires, at.along_y, chunk(0), chunk, rows_half)

    up.wait_recv()
    down.wait_recv()
    acc_ref[at.y] = acc_ref[at.y] + from_up_ref[...] + from_down_ref[...]
    far_rows = pl.ds(pl.multiple_of((1 - at.xh) * 128, 128), 128)
    own_rows = pl.ds(pl.multiple_of(at.xh * 128, 128), 128)
    across = wires.send(acc_ref.at[at.y, far_rows], far_ref, at.far_x())
    across.wait_recv()
    piece_ref[...] = (acc_ref[at.y, own_rows] + far_ref[...]).astype(jnp.bfloat16)

    def spot(x, z):
        q = z * 2 + lax.rem(x, 2)
        return pl.multiple_of(lax.div(x, 2) * 128, 128), pl.ds(pl.multiple_of(q * 256, 256), 256)

    def colour(n, x, z):
        row, cols = spot(x, z)
        return queries_ref.at[pl.ds(row + n * 64, 64), cols]

    row, cols = spot(at.x, at.z)
    queries_ref[pl.ds(row, 128), cols] = piece_ref[...]
    run_together(
        torus_gather(
            wires, at.along_x, at.along_z, piece_ref.at[0:64],
            lambda i, j: colour(0, ring(at.x, i), ring(at.z, j)), rows_half,
        ),
        torus_gather(
            wires, at.along_z, at.along_x, piece_ref.at[64:128],
            lambda i, j: colour(1, ring(at.x, j), ring(at.z, i)), rows_half,
        ),
    )
    book_end = ends[1][1]()
    ends[1][0]()
    book_end()
    codes_forward()()
    wires.drain()


VM = pl.BlockSpec(memory_space=pltpu.VMEM)


def exchange(slice_own, weight, codes, book_half):
    f32, b16 = jnp.float32, jnp.bfloat16
    return pl.pallas_call(
        exchange_kernel,
        in_specs=[VM] * 4,
        out_specs=[VM] * 4,
        out_shape=[
            jax.ShapeDtypeStruct((8, 128, 256), b16),
            jax.ShapeDtypeStruct((256, 2048), b16),
            jax.ShapeDtypeStruct((256, 2048), b16),
            jax.ShapeDtypeStruct((8, 256, 256), b16),
        ],
        scratch_shapes=[
            pltpu.VMEM((4, 256, 256), f32),
            pltpu.VMEM((4, 256, 256), f32),
            pltpu.VMEM((4, 256, 256), f32),
            pltpu.VMEM((128, 256), f32),
            pltpu.VMEM((128, 256), f32),
            pltpu.VMEM((256, 256), f32),
            pltpu.VMEM((256, 256), f32),
            pltpu.VMEM((128, 256), f32),
            pltpu.VMEM((128, 256), b16),
            pltpu.SemaphoreType.DMA((96,)),
            pltpu.SemaphoreType.DMA((96,)),
        ],
        compiler_params=pltpu.CompilerParams(collective_id=0, has_side_effects=True),
        name="exchange",
    )(slice_own, weight, codes, book_half)


def scores_kernel(
    queries_ref, passages_ref, column_ref, all_grad_ref, losses_ref,
    other_ref, came_ref, scores_ref, stat_ref, stats_ref, grad_ref,
    send_sems, recv_sems,
):
    at = Place()
    wires = Wires(send_sems, recv_sems)
    cells = [
        {"xh": lax.rem(at.xh + h, 2), **({} if not g else g)}
        for h in range(2)
        for g in [None] + at.group()
        if h or g
    ]
    greet([at.core()] + cells)
    there = pl.ds(pl.multiple_of((1 - at.k) * 128, 128), 128)
    here = pl.ds(pl.multiple_of(at.k * 128, 128), 128)
    parts = 4
    width = passages_ref.shape[1] // parts
    crossed = []
    for part in range(parts):
        cols = slice(part * width, (part + 1) * width)
        other_ref[:, cols] = jnp.dot(
            queries_ref[there, :], passages_ref[:, cols], preferred_element_type=jnp.float32
        )
        crossed.append(wires.send(other_ref.at[:, cols], came_ref.at[:, cols], at.core()))
    for part in range(parts):
        cols = slice(part * width, (part + 1) * width)
        scores_ref[:, cols] = jnp.dot(
            queries_ref[here, :], passages_ref[:, cols], preferred_element_type=jnp.float32
        )
    for copy in crossed:
        copy.wait_recv()
    scores = (scores_ref[...] + came_ref[...]) * score_scale
    scores_ref[...] = scores
    target = lax.broadcasted_iota(jnp.int32, scores.shape, 1) == column_ref[...]
    local_max = jnp.max(scores, axis=1, keepdims=True)
    positive = jnp.sum(jnp.where(target, scores, 0.0), axis=1, keepdims=True)
    local_total = jnp.sum(jnp.exp(scores - local_max), axis=1, keepdims=True)
    lane = lax.broadcasted_iota(jnp.int32, (128, 128), 1)
    packed = jnp.where(lane == 0, local_max, jnp.where(lane == 1, local_total, positive))
    mine = jnp.transpose(packed)[0:8, :]
    stat_ref[...] = mine
    slot = at.xh * 8 + at.qry
    copies = [wires.send(stat_ref, stats_ref.at[slot], cell) for cell in cells]
    stats_ref[slot] = mine
    for copy in copies:
        copy.wait_recv()
    high = stats_ref[0, 0:1, :]
    for n in range(1, 16):
        high = jnp.maximum(high, stats_ref[n, 0:1, :])
    total = jnp.zeros_like(high)
    hit = jnp.zeros_like(high)
    for n in range(16):
        total = total + stats_ref[n, 1:2, :] * jnp.exp(stats_ref[n, 0:1, :] - high)
        hit = hit + stats_ref[n, 2:3, :]
    losses_ref[...] = jnp.broadcast_to(jnp.log(total) + high - hit, (8, 128))
    row = lax.broadcasted_iota(jnp.int32, (128, 128), 0)
    back = jnp.transpose(jnp.where(row == 0, high, total))
    row_max, row_total = back[:, 0:1], back[:, 1:2]
    grad = jnp.exp(scores_ref[...] - row_max) / row_total - target.astype(jnp.float32)
    grad = grad.astype(jnp.bfloat16)
    grad_ref[...] = grad
    copy = wires.send(grad_ref, all_grad_ref.at[here], at.core())
    all_grad_ref[here, :] = grad
    copy.wait_recv()
    wires.drain()


def score_grads(queries, passages, column):
    f32, b16 = jnp.float32, jnp.bfloat16
    count = passages.shape[1]
    return pl.pallas_call(
        scores_kernel,
        in_specs=[VM] * 3,
        out_specs=[VM] * 2,
        out_shape=[jax.ShapeDtypeStruct((256, count), b16), jax.ShapeDtypeStruct((8, 128), f32)],
        scratch_shapes=[
            pltpu.VMEM((128, count), f32),
            pltpu.VMEM((128, count), f32),
            pltpu.VMEM((128, count), f32),
            pltpu.VMEM((8, 128), f32),
            pltpu.VMEM((16, 8, 128), f32),
            pltpu.VMEM((128, count), b16),
            pltpu.SemaphoreType.DMA((24,)),
            pltpu.SemaphoreType.DMA((24,)),
        ],
        compiler_params=pltpu.CompilerParams(collective_id=1, has_side_effects=True),
        name="score_grads",
    )(queries, passages, column)


def ring_sum(wires, along, block, half, came):
    def add(ref, *others):
        total = ref[...].astype(jnp.float32)
        for other in others:
            total = total + other[...].astype(jnp.float32)
        ref[...] = total.astype(ref.dtype)

    up_half, down_half, up_full, down_full = came
    up = wires.send(half(block(2), 0), up_half, along(1))
    down = wires.send(half(block(2), 1), down_half, along(-1))
    yield
    up.wait_recv()
    add(half(block(1), 0), up_half)
    up = wires.send(block(1), up_full, along(1))
    down.wait_recv()
    add(half(block(-1), 1), down_half)
    down = wires.send(block(-1), down_full, along(-1))
    yield
    up.wait_recv()
    down.wait_recv()
    add(block(0), up_full, down_full)


def middle_half(ref, side):
    rows = ref.shape[-2] // 2
    return ref.at[:, rows * side : rows * side + rows]


def grads_kernel(
    grad_ref, passages_ref, normed_ref, weight_ref, losses_ref, sums_ref,
    weight_grad_ref, norm_ref, losses_all_ref, book_ref,
    part_ref, x_half, x_full, z_half, z_full, piece_ref, query_ref, term_ref, terms_ref, norm_piece_ref,
    add_ref, y_half, y_full, share_ref, far_ref, final_ref,
    send_sems, recv_sems,
):
    at = Place()
    wires = Wires(send_sems, recv_sems)
    group = at.group()
    cells = [at.core()] + [{**at.along_y(s), "k": c} for s in (1, 2, 3) for c in (at.k, 1 - at.k)]
    greet(group + cells + [at.far_x(), {"xh": 1 - at.xh, "xl": 1 - at.xl}])
    places = at.y * 2 + at.k
    lost = [wires.send(losses_ref, losses_all_ref.at[places], cell) for cell in cells]
    losses_all_ref[places] = losses_ref[...]

    def book_sums_over_devices():
        add_ref[...] = sums_ref[...]
        yield from ring_sum(
            wires, at.along_y, lambda s: add_ref.at[ring(at.y, s)], middle_half,
            (y_half.at[0], y_half.at[1], y_full.at[0], y_full.at[1]),
        )
        copies = []
        for n, peer in enumerate(group):
            q = peer["z"] * 2 + peer["xl"]
            copies.append(wires.send(add_ref.at[at.y, q], share_ref.at[n], peer))
        yield
        total = add_ref[at.y, at.qry].astype(jnp.float32)
        for n, copy in enumerate(copies):
            copy.wait_recv()
            total = total + share_ref[n].astype(jnp.float32)
        final_ref[0] = total.astype(jnp.bfloat16)
        across = wires.send(final_ref.at[0], far_ref, at.far_x())
        yield
        across.wait_recv()
        whole = final_ref[0].astype(jnp.float32) + far_ref[...].astype(jnp.float32)
        final_ref[1] = whole.astype(jnp.bfloat16)

        def spot(s):
            return book_ref.at[at.k, ring(at.y, s)]

        forward = ring_gather(wires, at.along_y, final_ref.at[1], spot, rows_half)
        cores = [wires.send(final_ref.at[1], spot(0), at.core())]
        book_ref[at.k, at.y] = final_ref[1]
        yield
        finish = forward()
        for s in (-1, 1):
            cores.append(wires.send(spot(s), spot(s), at.core()))
        yield
        finish()
        cores.append(wires.send(spot(2), spot(2), at.core()))
        yield
        for copy in cores:
            copy.wait_recv()

    def main():
        for q in range(8):
            product = lax.dot_general(
                grad_ref[...], passages_ref[q * 256 : q * 256 + 256, :],
                (((1,), (1,)), ((), ())), preferred_element_type=jnp.float32,
            )
            z, xl = divmod(q, 2)
            for xh in range(2):
                x = xh * 2 + xl
                part_ref[0, x, z] = product[xh * 128 : xh * 128 + 128, 0:128]
                part_ref[1, z, x] = product[xh * 128 : xh * 128 + 128, 128:256]
        pair = [
            ring_sum(
                wires, along, lambda s, n=n, c=c: part_ref.at[n, ring(c, s)], middle_half,
                (x_half.at[n, 0], x_half.at[n, 1], x_full.at[n, 0], x_full.at[n, 1]),
            )
            for n, along, c in ((0, at.along_x, at.x), (1, at.along_z, at.z))
        ]
        yield from both(*pair)
        pair = [
            ring_sum(
                wires, along, lambda s, n=n, b=b, c=c: part_ref.at[n, b, ring(c, s)], rows_half,
                (z_half.at[n, 0], z_half.at[n, 1], z_full.at[n, 0], z_full.at[n, 1]),
            )
            for n, along, b, c in ((0, at.along_z, at.x, at.z), (1, at.along_x, at.z, at.x))
        ]
        yield from both(*pair)
        for n, b, c in ((0, at.x, at.z), (1, at.z, at.x)):
            piece_ref[:, n * 128 : n * 128 + 128] = (part_ref[n, b, c] * score_scale).astype(jnp.bfloat16)

        def spot(xh, y, k):
            return query_ref.at[
                pl.ds(pl.multiple_of(y * 256 + xh * 128, 128), 128),
                pl.ds(pl.multiple_of(k * 256, 256), 256),
            ]

        spot(at.xh, at.y, at.k)[...] = piece_ref[...]
        yield from psg_gather(wires, at, piece_ref, spot)
        for q in range(8):
            term_ref[q] = lax.dot_general(
                query_ref[q * 128 : q * 128 + 128, :], weight_ref[...],
                (((1,), (1,)), ((), ())), preferred_element_type=jnp.float32,
            ).astype(jnp.bfloat16)
        copies = []
        for n, peer in enumerate(group):
            q = peer["z"] * 2 + peer["xl"]
            copies.append(wires.send(term_ref.at[q], terms_ref.at[n], peer))
        weight_grad_ref[...] = lax.dot_general(
            normed_ref[...].reshape(1024, 256), query_ref[...],
            (((0,), (0,)), ((), ())), preferred_element_type=jnp.float32,
        )
        yield
        total = term_ref[at.qry].astype(jnp.float32)
        for n, copy in enumerate(copies):
            copy.wait_recv()
            total = total + terms_ref[n].astype(jnp.float32)
        norm_piece_ref[...] = total.astype(jnp.bfloat16)

        def column(xh, y, k):
            place = (xh * 4 + y) * 2 + k
            return norm_ref.at[:, pl.ds(pl.multiple_of(place * 256, 256), 256)]

        column(at.xh, at.y, at.k)[...] = norm_piece_ref[...]
        yield from psg_gather(wires, at, norm_piece_ref, column)

    run_together(main(), book_sums_over_devices())
    for copy in lost:
        copy.wait_recv()
    wires.drain()


def grads(all_grad, passages, normed, weight, losses, sums):
    f32, b16 = jnp.float32, jnp.bfloat16
    return pl.pallas_call(
        grads_kernel,
        in_specs=[VM] * 6,
        out_specs=[VM] * 4,
        out_shape=[
            jax.ShapeDtypeStruct((256, 512), f32),
            jax.ShapeDtypeStruct((128, 4096), b16),
            jax.ShapeDtypeStruct((8, 8, 128), f32),
            jax.ShapeDtypeStruct((2, 4, 64, 256), b16),
        ],
        scratch_shapes=[
            pltpu.VMEM((2, 4, 4, 128, 128), f32),
            pltpu.VMEM((2, 2, 4, 64, 128), f32),
            pltpu.VMEM((2, 2, 4, 128, 128), f32),
            pltpu.VMEM((2, 2, 64, 128), f32),
            pltpu.VMEM((2, 2, 128, 128), f32),
            pltpu.VMEM((128, 256), b16),
            pltpu.VMEM((1024, 512), b16),
            pltpu.VMEM((8, 128, 256), b16),
            pltpu.VMEM((7, 128, 256), b16),
            pltpu.VMEM((128, 256), b16),
            pltpu.VMEM((4, 8, 64, 256), b16),
            pltpu.VMEM((2, 8, 32, 256), b16),
            pltpu.VMEM((2, 8, 64, 256), b16),
            pltpu.VMEM((7, 64, 256), b16),
            pltpu.VMEM((64, 256), b16),
            pltpu.VMEM((2, 64, 256), b16),
            pltpu.SemaphoreType.DMA((112,)),
            pltpu.SemaphoreType.DMA((112,)),
        ],
        compiler_params=pltpu.CompilerParams(collective_id=2, has_side_effects=True),
        name="grads",
    )(all_grad, passages, normed, weight, losses, sums)


def unfold(sums):
    groups = sums.shape[0]
    parts = sums.reshape(groups, 64, 8, 4, 8)
    return parts.transpose(0, 2, 4, 3, 1).reshape(groups * 8, 8, 256)


def per_device(hidden, norm_gain, proj_weight, pq_codes, codebook, positives):
    xh, y, k = (lax.axis_index(a) for a in PSG)
    psg = (xh * 4 + y) * 2 + k
    qry = lax.axis_index("z") * 2 + lax.axis_index("xl")
    own_rows, width = hidden.shape
    row_span, columns = proj_weight.shape
    subs = pq_codes.shape[1]
    half = subs // 2
    held = pq_codes.shape[0]
    piece = held // 8

    floats = hidden.astype(jnp.float32)
    inverse = lax.rsqrt(jnp.mean(floats * floats, axis=1, keepdims=True) + norm_eps)
    normed_own = (floats * inverse * norm_gain[None, :]).astype(jnp.bfloat16)
    slice_own = lax.dynamic_slice_in_dim(normed_own, psg * row_span, row_span, 1)
    codes = pq_codes.T.astype(jnp.bfloat16)
    book_half = lax.dynamic_slice_in_dim(codebook, k * half, half, 0).reshape(half * 8, 256)
    normed, queries, codes, book = exchange(slice_own, proj_weight, codes, book_half)
    passages = decode(codes, book.reshape(2048, 256))

    block = y * 2 + k
    targets = lax.dynamic_slice_in_dim(positives, block * own_rows, own_rows, 0)
    shard = targets // held
    inside = targets - shard * held
    sixth = inside // piece
    here = (shard // 8 == xh) & (sixth == qry)
    column = jnp.where(here, (shard % 8) * piece + inside % piece, -1)
    all_grad, block_losses = score_grads(queries, passages, column[:, None])
    sums = book_sums(codes, queries, all_grad).astype(jnp.bfloat16)
    sums = sums.reshape(8, 4, 64, 256).transpose(1, 0, 2, 3)
    weight_grad, norm_back, all_losses, book_grad = grads(
        all_grad, passages, normed, proj_weight, block_losses, sums
    )
    losses = lax.dynamic_index_in_dim(all_losses, qry, 0, keepdims=False)[0]
    codebook_grad = unfold(book_grad.reshape(8, 64, 256).astype(jnp.float32))
    norm_back = norm_back.astype(jnp.float32)
    scaled = norm_back * norm_gain[None, :]
    hidden_grad = (
        inverse * scaled
        - floats
        * inverse
        * inverse
        * inverse
        * jnp.mean(scaled * floats, axis=1, keepdims=True)
    ).astype(jnp.bfloat16)
    return (losses, hidden_grad, weight_grad, codebook_grad)


def solution(mesh):
    split = Mesh(mesh.devices.reshape(2, 4, 2, 4, 2), AXES)
    return jax.shard_map(
        per_device,
        mesh=split,
        in_specs=(P(QRY, None), P(), P(PSG, QRY), P(PSG, QRY), P(QRY, None, None), P()),
        out_specs=(P(QRY), P(QRY, None), P(PSG, QRY), P(QRY, None, None)),
        check_vma=False,
    )
```

```python
import jax
import jax.numpy as jnp
from jax import lax
from jax.experimental import pallas as pl
from jax.experimental.pallas import tpu as pltpu
from jax.sharding import Mesh
from jax.sharding import PartitionSpec as P

AXES = ("xh", "y", "k", "z", "xl")
PSG = ("xh", "y", "k")
QRY = ("z", "xl")

score_scale = 0.0625
norm_eps = 1e-06


def decode_slice(g, codes_ref, book_ref, out_ref):
    f32 = jnp.float32
    block, part = lax.div(g, 2), lax.rem(g, 2)
    rows = pl.ds(pl.multiple_of(g * 16, 16), 16)
    books = []
    for pair in range(8):
        both_rows = book_ref[block, pl.ds(pl.multiple_of(part * 128 + pair * 16, 16), 16), :].astype(f32)
        books += [both_rows[0:8], both_rows[8:16]]

    def tile_step(tile, carry):
        at = pl.ds(pl.multiple_of(tile * 128, 128), 128)
        codes = codes_ref[rows, at].astype(f32).astype(jnp.int32)
        for pair in range(8):
            found = []
            for m in (pair * 2, pair * 2 + 1):
                code = jnp.broadcast_to(codes[m : m + 1, :], (8, 128))
                low = code & 127
                picked = [
                    jnp.take_along_axis(
                        books[m][:, half * 128 : half * 128 + 128], low, axis=1,
                        mode="promise_in_bounds",
                    )
                    for half in range(2)
                ]
                found.append(jnp.where(code >= 128, picked[1], picked[0]))
            out_ref[pl.ds(pl.multiple_of(g * 128 + pair * 16, 16), 16), at] = jnp.concatenate(
                found, 0
            ).astype(jnp.bfloat16)
        return carry

    lax.fori_loop(0, codes_ref.shape[1] // 128, tile_step, 0, unroll=16)


def split_codes(codes_ref, hi_ref, lo_ref):
    whole = codes_ref[...].astype(jnp.float32)
    lo = jnp.floor(whole * (1.0 / 64.0))
    lo_ref[...] = lo
    hi_ref[...] = whole - lo * 64.0

def book_block(b, hi_ref, lo_ref, queries_ref, grad_ref, pg_ref, hot_ref, gw_ref, put):
    b16, f32 = jnp.bfloat16, jnp.float32
    count = grad_ref.shape[1]
    pg_ref[...] = (
        lax.dot_general(
            queries_ref[:, pl.ds(pl.multiple_of(b * 256, 256), 256)], grad_ref[...],
            (((0,), (0,)), ((), ())), preferred_element_type=f32,
        ) * score_scale
    ).astype(b16)
    sublane = lax.broadcasted_iota(jnp.int32, (16, 128), 0).astype(f32)
    levels = [(sublane + 16.0 * j).astype(b16) for j in range(4)]
    upper = lax.broadcasted_iota(jnp.int32, (16, 128), 0) >= 8
    picks = [jnp.where(upper, 2.0 * j + 1.0, 2.0 * j).astype(b16) for j in range(2)]
    one, zero = jnp.ones((16, 128), b16), jnp.zeros((16, 128), b16)
    own = lax.div(lax.broadcasted_iota(jnp.int32, (64, 256), 1), 32)

    def group_step(group, carry):
        rows = pl.ds(pl.multiple_of(b * 32 + group * 8, 8), 8)

        def tile_step(tile, carry):
            at = pl.ds(pl.multiple_of(tile * 128, 128), 128)
            hi_block, lo_block = hi_ref[rows, at], lo_ref[rows, at]
            for pair in range(4):
                grads = pg_ref[pl.ds(pl.multiple_of(group * 64 + pair * 16, 16), 16), at].astype(f32)
                for side in range(2):
                    m = pair * 2 + side
                    hi = jnp.broadcast_to(hi_block[m : m + 1, :], (16, 128)).astype(b16)
                    lo = jnp.broadcast_to(lo_block[m : m + 1, :], (16, 128)).astype(b16)
                    for j in range(4):
                        hot_ref[m * 64 + j * 16 : m * 64 + j * 16 + 16, at] = jnp.where(hi == levels[j], one, zero)
                    one_grad = grads[side * 8 : side * 8 + 8]
                    twice = jnp.concatenate([one_grad, one_grad], 0).astype(b16)
                    for j in range(2):
                        gw_ref[m * 32 + j * 16 : m * 32 + j * 16 + 16, at] = jnp.where(lo == picks[j], twice, zero)
            return carry

        lax.fori_loop(0, count // 128, tile_step, 0, unroll=16)
        full = lax.dot_general(
            hot_ref[...], gw_ref[...], (((1,), (1,)), ((), ())), preferred_element_type=f32
        )
        total = full[0:64]
        for m in range(1, 8):
            total = jnp.where(own == m, full[m * 64 : m * 64 + 64], total)
        put(group, b, total.astype(b16))
        return carry

    lax.fori_loop(0, 4, group_step, 0)


def ring(c, step):
    return lax.rem(c + (step + 4), 4)


class Place:
    def __init__(self):
        self.xh, self.y, self.k, self.z, self.xl = (lax.axis_index(a) for a in AXES)
        self.x = self.xh * 2 + self.xl
        self.qry = self.z * 2 + self.xl

    def along_x(self, step):
        x = ring(self.x, step)
        return {"xh": lax.div(x, 2), "xl": lax.rem(x, 2)}

    def along_y(self, step):
        return {"y": ring(self.y, step)}

    def along_z(self, step):
        return {"z": ring(self.z, step)}

    def core(self):
        return {"k": 1 - self.k}

    def far_x(self):
        return {"xh": 1 - self.xh}

    def group(self):
        return [
            {"z": ring(self.z, s), "xl": lax.rem(self.xl + f, 2)}
            for s in range(4)
            for f in range(2)
            if s or f
        ]


def greet(peers):
    barrier = pltpu.get_barrier_semaphore()
    for peer in peers:
        pl.semaphore_signal(
            barrier, inc=1, device_id=peer, device_id_type=pl.DeviceIdType.MESH
        )
    pl.semaphore_wait(barrier, len(peers))


class Wires:
    def __init__(self, send_sems, recv_sems):
        self.send_sems, self.recv_sems, self.copies = send_sems, recv_sems, []

    def send(self, src, dst, peer):
        n = len(self.copies)
        copy = pltpu.make_async_remote_copy(
            src_ref=src,
            dst_ref=dst,
            send_sem=self.send_sems.at[n],
            recv_sem=self.recv_sems.at[n],
            device_id=peer,
            device_id_type=pl.DeviceIdType.MESH,
        )
        copy.start()
        self.copies.append(copy)
        return copy

    def drain(self):
        for copy in self.copies:
            copy.wait_send()


def ring_gather(wires, along, own, block, halves):
    first = (wires.send(own, block(0), along(1)), wires.send(own, block(0), along(-1)))

    def forward():
        first[0].wait_recv()
        up = wires.send(halves(block(-1), 0), halves(block(-1), 0), along(1))
        first[1].wait_recv()
        down = wires.send(halves(block(1), 1), halves(block(1), 1), along(-1))

        def finish():
            up.wait_recv()
            down.wait_recv()

        return finish

    return forward


def torus_gather(wires, one, two, own, block, halves):
    forward = ring_gather(wires, one, own, lambda i: block(i, 0), halves)
    rest = [ring_gather(wires, two, own, lambda j: block(0, j), halves)]
    yield
    finish = forward()
    for i in (-1, 1):
        rest.append(
            ring_gather(wires, two, block(i, 0), lambda j, i=i: block(i, j), halves)
        )
    yield
    ends = [rest[0]()]
    finish()
    rest.append(ring_gather(wires, two, block(2, 0), lambda j: block(2, j), halves))
    yield
    ends += [r() for r in rest[1:3]]
    yield
    ends.append(rest[3]())
    for end in ends:
        end()


def both(*parts):
    live = list(parts)
    while live:
        live = [p for p in live if next(p, live) is not live]
        yield


def psg_gather(wires, at, own, block):
    def halves(ref, side):
        rows = ref.shape[0] // 2
        return ref.at[rows * side : rows * side + rows]

    def near(s):
        return block(at.xh, ring(at.y, s), at.k)

    def far(s):
        return block(1 - at.xh, ring(at.y, s), at.k)

    across = wires.send(own, near(0), at.far_x())
    forward = ring_gather(wires, at.along_y, own, near, halves)
    cores = [wires.send(own, near(0), at.core())]
    yield
    across.wait_recv()
    forward_far = ring_gather(wires, at.along_y, far(0), far, halves)
    cores.append(wires.send(far(0), far(0), at.core()))
    yield
    finish = forward()
    for s in (-1, 1):
        cores.append(wires.send(near(s), near(s), at.core()))
    yield
    finish_far = forward_far()
    for s in (-1, 1):
        cores.append(wires.send(far(s), far(s), at.core()))
    yield
    finish()
    cores.append(wires.send(near(2), near(2), at.core()))
    finish_far()
    cores.append(wires.send(far(2), far(2), at.core()))
    for copy in cores:
        copy.wait_recv()


def rows_half(ref, side):
    rows = ref.shape[-2] // 2
    return ref.at[rows * side : rows * side + rows]


def in_turns(order, **parts):
    live = set(parts)
    for name in list(order) + sorted(parts) * 64:
        if name in live and next(parts[name], live) is live:
            live.remove(name)


def exchange_kernel(
    slice_ref, weight_ref, codes_ref, book_ref,
    normed_ref, queries_ref, codes_all_ref, passages_ref,
    book_all_ref, other_ref, came_ref, acc_ref, up_ref, down_ref, from_up_ref, from_down_ref, far_ref, piece_ref,
    send_sems, recv_sems,
):
    at = Place()
    wires = Wires(send_sems, recv_sems)
    group = at.group()
    greet(
        group
        + [{"k": 1 - at.k, **g} for g in group]
        + [at.core(), at.along_y(1), at.along_y(-1), at.far_x()]
        + [{"xh": 1 - at.xh, "xl": 1 - at.xl}]
    )

    def column(ref, flip):
        return lambda s: ref.at[ring(at.z, s) * 2 + (at.xl if flip == 0 else 1 - at.xl)]

    def group_gather(own, out):
        near, far = column(out, 0), column(out, 1)
        side = wires.send(own, out.at[at.qry], {"xl": 1 - at.xl})
        forward = ring_gather(wires, at.along_z, own, near, rows_half)
        out[at.qry] = own[...]
        yield
        side.wait_recv()
        forward_far = ring_gather(wires, at.along_z, far(0), far, rows_half)
        yield
        finish = forward()
        yield
        finish_far = forward_far()
        yield
        finish()
        finish_far()

    def main():
        yield from group_gather(slice_ref, normed_ref)
        order = (2, 1, -1, 0)
        crossed = []
        for s in order:
            b = ring(at.y, s)
            left = normed_ref[pl.ds(b * 2, 2)].reshape(256, 256)
            other_ref[b] = jnp.dot(
                left,
                weight_ref[:, pl.ds(pl.multiple_of((1 - at.k) * 256, 256), 256)],
                preferred_element_type=jnp.float32,
            )
            crossed.append(wires.send(other_ref.at[b], came_ref.at[b], at.core()))
        for s in order:
            b = ring(at.y, s)
            left = normed_ref[pl.ds(b * 2, 2)].reshape(256, 256)
            acc_ref[b] = jnp.dot(
                left,
                weight_ref[:, pl.ds(pl.multiple_of(at.k * 256, 256), 256)],
                preferred_element_type=jnp.float32,
            )
        far_y, next_y, last_y = ring(at.y, 2), ring(at.y, 1), ring(at.y, -1)
        crossed[0].wait_recv()
        acc_ref[far_y] = acc_ref[far_y] + came_ref[far_y]
        up = wires.send(acc_ref.at[far_y, 0:128], up_ref, at.along_y(1))
        down = wires.send(acc_ref.at[far_y, 128:256], down_ref, at.along_y(-1))
        crossed[1].wait_recv()
        acc_ref[next_y] = acc_ref[next_y] + came_ref[next_y]
        crossed[2].wait_recv()
        acc_ref[last_y] = acc_ref[last_y] + came_ref[last_y]
        crossed[3].wait_recv()
        acc_ref[at.y] = acc_ref[at.y] + came_ref[at.y]
        yield
        up.wait_recv()
        acc_ref[next_y, 0:128] = acc_ref[next_y, 0:128] + up_ref[...]
        up = wires.send(acc_ref.at[next_y], from_up_ref, at.along_y(1))
        down.wait_recv()
        acc_ref[last_y, 128:256] = acc_ref[last_y, 128:256] + down_ref[...]
        down = wires.send(acc_ref.at[last_y], from_down_ref, at.along_y(-1))
        yield
        up.wait_recv()
        down.wait_recv()
        acc_ref[at.y] = acc_ref[at.y] + from_up_ref[...] + from_down_ref[...]
        far_rows = pl.ds(pl.multiple_of((1 - at.xh) * 128, 128), 128)
        own_rows = pl.ds(pl.multiple_of(at.xh * 128, 128), 128)
        across = wires.send(acc_ref.at[at.y, far_rows], far_ref, at.far_x())
        yield
        across.wait_recv()
        piece_ref[...] = (acc_ref[at.y, own_rows] + far_ref[...]).astype(jnp.bfloat16)

        def spot(x, z):
            q = z * 2 + lax.rem(x, 2)
            row = pl.multiple_of(lax.div(x, 2) * 128, 128)
            return row, pl.ds(pl.multiple_of(q * 256, 256), 256)

        def colour(n, x, z):
            row, cols = spot(x, z)
            return queries_ref.at[pl.ds(row + n * 64, 64), cols]

        row, cols = spot(at.x, at.z)
        queries_ref[pl.ds(row, 128), cols] = piece_ref[...]
        yield from both(
            torus_gather(
                wires, at.along_x, at.along_z, piece_ref.at[0:64],
                lambda i, j: colour(0, ring(at.x, i), ring(at.z, j)), rows_half,
            ),
            torus_gather(
                wires, at.along_z, at.along_x, piece_ref.at[64:128],
                lambda i, j: colour(1, ring(at.x, j), ring(at.z, i)), rows_half,
            ),
        )

    def codes_chain():
        sent = []
        mine = pl.ds(pl.multiple_of(at.y * 512 + at.k * 256, 256), 256)
        rows_here = pl.ds(pl.multiple_of(at.qry * 32, 32), 32)
        for cross in range(2):
            k = at.k if cross == 0 else 1 - at.k
            rows_there = pl.ds(pl.multiple_of(k * 32, 32), 32)
            for peer in ([] if cross == 0 else [{}]) + group:
                q = peer["z"] * 2 + peer["xl"] if peer else at.qry
                sent.append(
                    wires.send(
                        codes_ref.at[rows_there, pl.ds(pl.multiple_of(q * 256, 256), 256)],
                        codes_all_ref.at[rows_here, mine],
                        {"k": k, **peer},
                    )
                )
        codes_all_ref[rows_here, mine] = codes_ref[
            pl.ds(pl.multiple_of(at.k * 32, 32), 32),
            pl.ds(pl.multiple_of(at.qry * 256, 256), 256),
        ]
        yield
        for copy in sent:
            copy.wait_recv()

        def chunk(s):
            return codes_all_ref.at[:, pl.ds(pl.multiple_of(ring(at.y, s) * 512, 512), 512)]

        forward = ring_gather(wires, at.along_y, chunk(0), chunk, rows_half)
        yield
        finish = forward()
        yield
        finish()

    def decoded():
        for g in range(0, 16, 2):

            def step(n, carry):
                decode_slice(n, codes_all_ref, book_all_ref, passages_ref)
                return carry

            lax.fori_loop(g, g + 2, step, 0)
            yield

    in_turns(
        EXCHANGE_ORDER,
        m=main(), c=codes_chain(), b=group_gather(book_ref, book_all_ref), d=decoded(),
    )
    wires.drain()


EXCHANGE_ORDER = "mc" + "m" + "m" + "c" + "m" + "b" + "m" + "b" + "c" + "bb" + "m" + "bc" + "d" + "m" + "d" + "m" + "dmdmdmdmdmdm"


VM = pl.BlockSpec(memory_space=pltpu.VMEM)


def exchange(slice_own, weight, codes, book_half):
    f32, b16 = jnp.float32, jnp.bfloat16
    return pl.pallas_call(
        exchange_kernel,
        in_specs=[VM] * 4,
        out_specs=[VM] * 4,
        out_shape=[
            jax.ShapeDtypeStruct((8, 128, 256), b16),
            jax.ShapeDtypeStruct((256, 2048), b16),
            jax.ShapeDtypeStruct((256, 2048), b16),
            jax.ShapeDtypeStruct((2048, 2048), b16),
        ],
        scratch_shapes=[
            pltpu.VMEM((8, 256, 256), b16),
            pltpu.VMEM((4, 256, 256), f32),
            pltpu.VMEM((4, 256, 256), f32),
            pltpu.VMEM((4, 256, 256), f32),
            pltpu.VMEM((128, 256), f32),
            pltpu.VMEM((128, 256), f32),
            pltpu.VMEM((256, 256), f32),
            pltpu.VMEM((256, 256), f32),
            pltpu.VMEM((128, 256), f32),
            pltpu.VMEM((128, 256), b16),
            pltpu.SemaphoreType.DMA((96,)),
            pltpu.SemaphoreType.DMA((96,)),
        ],
        compiler_params=pltpu.CompilerParams(collective_id=0, has_side_effects=True),
        name="exchange",
    )(slice_own, weight, codes, book_half)


def scores_kernel(
    queries_ref, passages_ref, column_ref, all_grad_ref, losses_ref,
    other_ref, came_ref, scores_ref, stat_ref, stats_ref, grad_ref,
    send_sems, recv_sems,
):
    at = Place()
    wires = Wires(send_sems, recv_sems)
    cells = [
        {"xh": lax.rem(at.xh + h, 2), **({} if not g else g)}
        for h in range(2)
        for g in [None] + at.group()
        if h or g
    ]
    greet([at.core()] + cells)
    there = pl.ds(pl.multiple_of((1 - at.k) * 128, 128), 128)
    here = pl.ds(pl.multiple_of(at.k * 128, 128), 128)
    parts = 4
    width = passages_ref.shape[1] // parts
    crossed = []
    for part in range(parts):
        cols = slice(part * width, (part + 1) * width)
        other_ref[:, cols] = jnp.dot(
            queries_ref[there, :], passages_ref[:, cols], preferred_element_type=jnp.float32
        )
        crossed.append(wires.send(other_ref.at[:, cols], came_ref.at[:, cols], at.core()))
    for part in range(parts):
        cols = slice(part * width, (part + 1) * width)
        scores_ref[:, cols] = jnp.dot(
            queries_ref[here, :], passages_ref[:, cols], preferred_element_type=jnp.float32
        )
    for copy in crossed:
        copy.wait_recv()
    scores = (scores_ref[...] + came_ref[...]) * score_scale
    scores_ref[...] = scores
    target = lax.broadcasted_iota(jnp.int32, scores.shape, 1) == column_ref[...]
    local_max = jnp.max(scores, axis=1, keepdims=True)
    positive = jnp.sum(jnp.where(target, scores, 0.0), axis=1, keepdims=True)
    local_total = jnp.sum(jnp.exp(scores - local_max), axis=1, keepdims=True)
    lane = lax.broadcasted_iota(jnp.int32, (128, 128), 1)
    packed = jnp.where(lane == 0, local_max, jnp.where(lane == 1, local_total, positive))
    mine = jnp.transpose(packed)[0:8, :]
    stat_ref[...] = mine
    slot = at.xh * 8 + at.qry
    copies = [wires.send(stat_ref, stats_ref.at[slot], cell) for cell in cells]
    stats_ref[slot] = mine
    for copy in copies:
        copy.wait_recv()
    high = stats_ref[0, 0:1, :]
    for n in range(1, 16):
        high = jnp.maximum(high, stats_ref[n, 0:1, :])
    total = jnp.zeros_like(high)
    hit = jnp.zeros_like(high)
    for n in range(16):
        total = total + stats_ref[n, 1:2, :] * jnp.exp(stats_ref[n, 0:1, :] - high)
        hit = hit + stats_ref[n, 2:3, :]
    losses_ref[...] = jnp.broadcast_to(jnp.log(total) + high - hit, (8, 128))
    row = lax.broadcasted_iota(jnp.int32, (128, 128), 0)
    back = jnp.transpose(jnp.where(row == 0, high, total))
    row_max, row_total = back[:, 0:1], back[:, 1:2]
    grad = jnp.exp(scores_ref[...] - row_max) / row_total - target.astype(jnp.float32)
    grad = grad.astype(jnp.bfloat16)
    grad_ref[...] = grad
    copy = wires.send(grad_ref, all_grad_ref.at[here], at.core())
    all_grad_ref[here, :] = grad
    copy.wait_recv()
    wires.drain()


def score_grads(queries, passages, column):
    f32, b16 = jnp.float32, jnp.bfloat16
    count = passages.shape[1]
    return pl.pallas_call(
        scores_kernel,
        in_specs=[VM] * 3,
        out_specs=[VM] * 2,
        out_shape=[jax.ShapeDtypeStruct((256, count), b16), jax.ShapeDtypeStruct((8, 128), f32)],
        scratch_shapes=[
            pltpu.VMEM((128, count), f32),
            pltpu.VMEM((128, count), f32),
            pltpu.VMEM((128, count), f32),
            pltpu.VMEM((8, 128), f32),
            pltpu.VMEM((16, 8, 128), f32),
            pltpu.VMEM((128, count), b16),
            pltpu.SemaphoreType.DMA((24,)),
            pltpu.SemaphoreType.DMA((24,)),
        ],
        compiler_params=pltpu.CompilerParams(collective_id=1, has_side_effects=True),
        name="score_grads",
    )(queries, passages, column)


def ring_sum(wires, along, block, half, came):
    def add(ref, *others):
        total = ref[...].astype(jnp.float32)
        for other in others:
            total = total + other[...].astype(jnp.float32)
        ref[...] = total.astype(ref.dtype)

    up_half, down_half, up_full, down_full = came
    up = wires.send(half(block(2), 0), up_half, along(1))
    down = wires.send(half(block(2), 1), down_half, along(-1))
    yield
    up.wait_recv()
    add(half(block(1), 0), up_half)
    up = wires.send(block(1), up_full, along(1))
    down.wait_recv()
    add(half(block(-1), 1), down_half)
    down = wires.send(block(-1), down_full, along(-1))
    yield
    up.wait_recv()
    down.wait_recv()
    add(block(0), up_full, down_full)


def middle_half(ref, side):
    rows = ref.shape[-2] // 2
    return ref.at[:, rows * side : rows * side + rows]


def grads_kernel(
    grad_ref, passages_ref, normed_ref, weight_ref, losses_ref, codes_ref, queries_ref,
    weight_grad_ref, norm_ref, losses_all_ref, book_ref,
    part_ref, x_half, x_full, z_half, z_full, piece_ref, query_ref, term_ref, terms_ref, norm_piece_ref,
    add_ref, y_half, y_full, share_ref, far_ref, final_ref, hi_ref, lo_ref, pg_ref, hot_ref, gw_ref,
    send_sems, recv_sems,
):
    at = Place()
    wires = Wires(send_sems, recv_sems)
    group = at.group()
    cells = [at.core()] + [{**at.along_y(s), "k": c} for s in (1, 2, 3) for c in (at.k, 1 - at.k)]
    greet(group + cells + [at.far_x(), {"xh": 1 - at.xh, "xl": 1 - at.xl}])
    places = at.y * 2 + at.k
    lost = [wires.send(losses_ref, losses_all_ref.at[places], cell) for cell in cells]
    losses_all_ref[places] = losses_ref[...]

    def book_sums_over_devices():
        def put(group, b, sums):
            add_ref[group, b] = sums

        split_codes(codes_ref, hi_ref, lo_ref)
        for b in range(8):
            book_block(
                b, hi_ref, lo_ref, queries_ref, grad_ref, pg_ref, hot_ref, gw_ref, put
            )
            yield
        yield from ring_sum(
            wires, at.along_y, lambda s: add_ref.at[ring(at.y, s)], middle_half,
            (y_half.at[0], y_half.at[1], y_full.at[0], y_full.at[1]),
        )
        copies = []
        for n, peer in enumerate(group):
            q = peer["z"] * 2 + peer["xl"]
            copies.append(wires.send(add_ref.at[at.y, q], share_ref.at[n], peer))
        yield
        total = add_ref[at.y, at.qry].astype(jnp.float32)
        for n, copy in enumerate(copies):
            copy.wait_recv()
            total = total + share_ref[n].astype(jnp.float32)
        final_ref[0] = total.astype(jnp.bfloat16)
        across = wires.send(final_ref.at[0], far_ref, at.far_x())
        yield
        across.wait_recv()
        whole = final_ref[0].astype(jnp.float32) + far_ref[...].astype(jnp.float32)
        final_ref[1] = whole.astype(jnp.bfloat16)

        def spot(s):
            return book_ref.at[at.k, ring(at.y, s)]

        forward = ring_gather(wires, at.along_y, final_ref.at[1], spot, rows_half)
        cores = [wires.send(final_ref.at[1], spot(0), at.core())]
        book_ref[at.k, at.y] = final_ref[1]
        yield
        finish = forward()
        for s in (-1, 1):
            cores.append(wires.send(spot(s), spot(s), at.core()))
        yield
        finish()
        cores.append(wires.send(spot(2), spot(2), at.core()))
        yield
        for copy in cores:
            copy.wait_recv()

    def main():
        for q in range(8):
            product = lax.dot_general(
                grad_ref[...], passages_ref[q * 256 : q * 256 + 256, :],
                (((1,), (1,)), ((), ())), preferred_element_type=jnp.float32,
            )
            z, xl = divmod(q, 2)
            for xh in range(2):
                x = xh * 2 + xl
                part_ref[0, x, z] = product[xh * 128 : xh * 128 + 128, 0:128]
                part_ref[1, z, x] = product[xh * 128 : xh * 128 + 128, 128:256]
        pair = [
            ring_sum(
                wires, along, lambda s, n=n, c=c: part_ref.at[n, ring(c, s)], middle_half,
                (x_half.at[n, 0], x_half.at[n, 1], x_full.at[n, 0], x_full.at[n, 1]),
            )
            for n, along, c in ((0, at.along_x, at.x), (1, at.along_z, at.z))
        ]
        yield from both(*pair)
        pair = [
            ring_sum(
                wires, along, lambda s, n=n, b=b, c=c: part_ref.at[n, b, ring(c, s)], rows_half,
                (z_half.at[n, 0], z_half.at[n, 1], z_full.at[n, 0], z_full.at[n, 1]),
            )
            for n, along, b, c in ((0, at.along_z, at.x, at.z), (1, at.along_x, at.z, at.x))
        ]
        yield from both(*pair)
        for n, b, c in ((0, at.x, at.z), (1, at.z, at.x)):
            piece_ref[:, n * 128 : n * 128 + 128] = (part_ref[n, b, c] * score_scale).astype(jnp.bfloat16)

        def spot(xh, y, k):
            return query_ref.at[
                pl.ds(pl.multiple_of(y * 256 + xh * 128, 128), 128),
                pl.ds(pl.multiple_of(k * 256, 256), 256),
            ]

        spot(at.xh, at.y, at.k)[...] = piece_ref[...]
        yield from psg_gather(wires, at, piece_ref, spot)
        for q in range(8):
            term_ref[q] = lax.dot_general(
                query_ref[q * 128 : q * 128 + 128, :], weight_ref[...],
                (((1,), (1,)), ((), ())), preferred_element_type=jnp.float32,
            ).astype(jnp.bfloat16)
        copies = []
        for n, peer in enumerate(group):
            q = peer["z"] * 2 + peer["xl"]
            copies.append(wires.send(term_ref.at[q], terms_ref.at[n], peer))
        weight_grad_ref[...] = lax.dot_general(
            normed_ref[...].reshape(1024, 256), query_ref[...],
            (((0,), (0,)), ((), ())), preferred_element_type=jnp.float32,
        )
        yield
        total = term_ref[at.qry].astype(jnp.float32)
        for n, copy in enumerate(copies):
            copy.wait_recv()
            total = total + terms_ref[n].astype(jnp.float32)
        norm_piece_ref[...] = total.astype(jnp.bfloat16)

        def column(xh, y, k):
            place = (xh * 4 + y) * 2 + k
            return norm_ref.at[:, pl.ds(pl.multiple_of(place * 256, 256), 256)]

        column(at.xh, at.y, at.k)[...] = norm_piece_ref[...]
        yield from psg_gather(wires, at, norm_piece_ref, column)

    in_turns(GRADS_ORDER, m=main(), b=book_sums_over_devices())
    for copy in lost:
        copy.wait_recv()
    wires.drain()


GRADS_ORDER = "mb" + "mbb" + "mb" + "mb" + "mb" + "mb" + "mb" + "bmbmbmbmbmbmbmbmb"


def grads(all_grad, passages, normed, weight, losses, codes, queries):
    f32, b16 = jnp.float32, jnp.bfloat16
    return pl.pallas_call(
        grads_kernel,
        in_specs=[VM] * 7,
        out_specs=[VM] * 4,
        out_shape=[
            jax.ShapeDtypeStruct((256, 512), f32),
            jax.ShapeDtypeStruct((128, 4096), b16),
            jax.ShapeDtypeStruct((8, 8, 128), f32),
            jax.ShapeDtypeStruct((2, 4, 64, 256), b16),
        ],
        scratch_shapes=[
            pltpu.VMEM((2, 4, 4, 128, 128), f32),
            pltpu.VMEM((2, 2, 4, 64, 128), f32),
            pltpu.VMEM((2, 2, 4, 128, 128), f32),
            pltpu.VMEM((2, 2, 64, 128), f32),
            pltpu.VMEM((2, 2, 128, 128), f32),
            pltpu.VMEM((128, 256), b16),
            pltpu.VMEM((1024, 512), b16),
            pltpu.VMEM((8, 128, 256), b16),
            pltpu.VMEM((7, 128, 256), b16),
            pltpu.VMEM((128, 256), b16),
            pltpu.VMEM((4, 8, 64, 256), b16),
            pltpu.VMEM((2, 8, 32, 256), b16),
            pltpu.VMEM((2, 8, 64, 256), b16),
            pltpu.VMEM((7, 64, 256), b16),
            pltpu.VMEM((64, 256), b16),
            pltpu.VMEM((2, 64, 256), b16),
            pltpu.VMEM((256, 2048), f32),
            pltpu.VMEM((256, 2048), f32),
            pltpu.VMEM((256, 2048), b16),
            pltpu.VMEM((512, 2048), b16),
            pltpu.VMEM((256, 2048), b16),
            pltpu.SemaphoreType.DMA((112,)),
            pltpu.SemaphoreType.DMA((112,)),
        ],
        compiler_params=pltpu.CompilerParams(collective_id=2, has_side_effects=True),
        name="grads",
    )(all_grad, passages, normed, weight, losses, codes, queries)


def unfold(sums):
    groups = sums.shape[0]
    parts = sums.reshape(groups, 64, 8, 4, 8)
    return parts.transpose(0, 2, 4, 3, 1).reshape(groups * 8, 8, 256)


def per_device(hidden, norm_gain, proj_weight, pq_codes, codebook, positives):
    xh, y, k = (lax.axis_index(a) for a in PSG)
    psg = (xh * 4 + y) * 2 + k
    qry = lax.axis_index("z") * 2 + lax.axis_index("xl")
    own_rows, width = hidden.shape
    row_span, columns = proj_weight.shape
    subs = pq_codes.shape[1]
    half = subs // 2
    held = pq_codes.shape[0]
    piece = held // 8

    floats = hidden.astype(jnp.float32)
    inverse = lax.rsqrt(jnp.mean(floats * floats, axis=1, keepdims=True) + norm_eps)
    normed_own = (floats * inverse * norm_gain[None, :]).astype(jnp.bfloat16)
    slice_own = lax.dynamic_slice_in_dim(normed_own, psg * row_span, row_span, 1)
    codes = pq_codes.T.astype(jnp.bfloat16)
    book_half = lax.dynamic_slice_in_dim(codebook, k * half, half, 0).reshape(half * 8, 256)
    normed, queries, codes, passages = exchange(slice_own, proj_weight, codes, book_half)

    block = y * 2 + k
    targets = lax.dynamic_slice_in_dim(positives, block * own_rows, own_rows, 0)
    shard = targets // held
    inside = targets - shard * held
    sixth = inside // piece
    here = (shard // 8 == xh) & (sixth == qry)
    column = jnp.where(here, (shard % 8) * piece + inside % piece, -1)
    all_grad, block_losses = score_grads(queries, passages, column[:, None])
    weight_grad, norm_back, all_losses, book_grad = grads(
        all_grad, passages, normed, proj_weight, block_losses, codes, queries
    )
    losses = lax.dynamic_index_in_dim(all_losses, qry, 0, keepdims=False)[0]
    codebook_grad = unfold(book_grad.reshape(8, 64, 256).astype(jnp.float32))
    norm_back = norm_back.astype(jnp.float32)
    scaled = norm_back * norm_gain[None, :]
    hidden_grad = (
        inverse * scaled
        - floats
        * inverse
        * inverse
        * inverse
        * jnp.mean(scaled * floats, axis=1, keepdims=True)
    ).astype(jnp.bfloat16)
    return (losses, hidden_grad, weight_grad, codebook_grad)


def solution(mesh):
    split = Mesh(mesh.devices.reshape(2, 4, 2, 4, 2), AXES)
    return jax.shard_map(
        per_device,
        mesh=split,
        in_specs=(P(QRY, None), P(), P(PSG, QRY), P(PSG, QRY), P(QRY, None, None), P()),
        out_specs=(P(QRY), P(QRY, None), P(PSG, QRY), P(QRY, None, None)),
        check_vma=False,
    )
```
